32 devices in a mesh: dp: 4 (over y, x), expert: 8 (over z, core).
Axes of the slice: x: 2, y: 2, z: 4, core: 2. Of those that a mesh axis runs over, the one named last changes fastest.
Arguments:
- tokens: bfloat16 [16384, 2048], P(('dp', 'expert')), may hold values from -6 to 6
- expert_ids: int32 [16384, 1], P(('dp', 'expert')), may hold values from 0 to 7; in each aligned block of 512 rows (0 to 511, 512 to 1023, ...) at most 128 rows name the same one
- gate_proj: bfloat16 [8, 2048, 768], P('expert'), may hold values from -0.125 to 0.125
- up_proj: bfloat16 [8, 2048, 768], P('expert'), may hold values from -0.125 to 0.125
- down_proj: bfloat16 [8, 768, 2048], P('expert'), may hold values from -0.21875 to 0.21875
Outputs:
- mixed: bfloat16 [16384, 2048], P(('dp', 'expert'))
- slot_index: int32 [16384], P(('dp', 'expert'))
The draws below stay inside these ranges and needn't reach their ends.
Inputs may be any that keep to these rules, and one draw needn't show every extreme that they name: `expert_ids`: among the rows of one device no expert is named more than 128 times; in some devices' rows one expert is named exactly 128 times.
All inputs are finite; a program needn't handle non-finite values.
Results may differ from the reference program's by a relative error of at most 0.0046.
The reference program's roundings to bfloat16 on the way (of `hidden`) count: a program that leaves them out, or rounds other values in their place, can miss the bound.
Values may be sent and summed in bfloat16 or wider, within the bound.
A program may use at most 64 MiB of HBM per device.

```python
import math
import jax
import jax.numpy as jnp
import numpy as np
from jax import lax

D = 2048
FF = 768
TOK_DEV = 512
EXPERTS = 8
TOKENS = 16384
MOST = 128
CAP = 2048


def block_scale(own_key, dims, pieces, least, high):
    loudness, own = 1.0, jax.random.fold_in(own_key, 6)
    for position, blocks in pieces:
        draws = jnp.exp(jax.random.uniform(jax.random.fold_in(own, position), (blocks,), jnp.float32, least / len(pieces), high / len(pieces)))
        loudness = loudness * jnp.repeat(draws, dims[position] // blocks).reshape([-1 if axis == position else 1 for axis in range(len(dims))])
    return loudness


def routed_block(stream_key, own, number, rows, number_of, top, reach, lean):
    sequence = jax.random.permutation(stream_key, number_of)
    crowded, common = portions_of(number_of, rows * top, reach, lean, True), portions_of(number_of, rows * top, reach, lean, False)
    places = jnp.arange(number_of)

    def named(sizes, turn):
        used = int((sizes > 0).sum())
        fixed = max(1, used // 4)
        shifted = fixed + (places - fixed + turn * (used - fixed)) % max(1, number_of - fixed)
        return jnp.zeros((number_of,), jnp.int32).at[sequence[jnp.where(places < fixed, places, shifted)]].set(jnp.asarray(sizes, jnp.int32))

    sizes = jnp.where(number % 4 == 0, named(crowded, number // 4), named(common, number - number // 4 - 1))
    mixed = jax.random.permutation(jax.random.fold_in(own, 3), number_of)
    donor, taker = mixed[0:number_of // 2 * 2:2], mixed[1:number_of // 2 * 2:2]
    slack = jnp.minimum(sizes[donor] - 1, reach - sizes[taker]) // 2
    slack = jnp.where((donor == sequence[0]) | (taker == sequence[0]) | (sizes[taker] == 0), 0, jnp.maximum(slack, 0))
    shifted = jax.random.randint(jax.random.fold_in(own, 4), (number_of // 2,), 0, 1 << 20) % (slack + 1)
    sizes = sizes.at[donor].add(-shifted).at[taker].add(shifted)
    items = jnp.searchsorted(jnp.cumsum(sizes), jnp.arange(rows * top), side="right").astype(jnp.int32)
    table = items.reshape(top, rows).T
    table = table[jax.random.permutation(jax.random.fold_in(own, 1), rows)]
    turn = jax.random.randint(jax.random.fold_in(own, 2), (rows, 1), 0, top)
    return jnp.take_along_axis(table, (jnp.arange(top)[None, :] + turn) % top, axis=1)


def portions_of(number_of, total, most, slope, full):
    weights = [(1 << 20) // math.isqrt(standing ** slope) + 1 for standing in range(1, number_of + 1)]
    largest = most if full else min(most, max(-(-total // number_of), total * weights[0] // sum(weights)))
    least = 1 if total - largest >= number_of - 1 else 0
    holding, rest = [largest] + [least] * (number_of - 1), total - largest - least * (number_of - 1)
    while rest > 0:
        candidates = [i for i in range(1, number_of) if holding[i] < largest] or [i for i in range(1, number_of) if holding[i] < most]
        pool, left = sum([weights[i] for i in candidates]), rest
        for i in candidates:
            more = min(most - holding[i], max(1, left * weights[i] // pool), rest)
            holding[i] = holding[i] + more
            rest = rest - more
    return np.array(holding)


def scatter_about(key, dims, spread, bound, cuts=(), kind=jnp.bfloat16):
    factor_of = block_scale(key, dims, cuts, -0.22, 0.18) if cuts else 1.0
    result = jax.random.normal(key, dims, jnp.float32) * spread * factor_of
    return jnp.minimum(jnp.maximum(result, -bound), bound).astype(kind)


def setup_inputs(seed: int = 0) -> dict:
    arg_keys = jax.random.split(jax.random.key(seed), 6)
    tokens = scatter_about(arg_keys[0], (TOKENS, D), 1.0, 6.0, ((0, 32),))
    expert_ids_keys = jax.random.split(jax.random.fold_in(arg_keys[1], 1), TOKENS // TOK_DEV)
    expert_ids_turns = jax.random.permutation(jax.random.fold_in(arg_keys[1], 3), TOKENS // TOK_DEV)
    expert_ids = jax.vmap(lambda own, number: routed_block(jax.random.fold_in(arg_keys[1], 2), own, number, TOK_DEV, EXPERTS, 1, MOST, 2))(expert_ids_keys, expert_ids_turns).reshape((TOKENS, 1))
    gate_proj = scatter_about(arg_keys[2], (EXPERTS, D, FF), D ** -0.5, 0.125, ((0, 8),))
    up_proj = scatter_about(arg_keys[3], (EXPERTS, D, FF), D ** -0.5, 0.125, ((0, 8),))
    down_proj = scatter_about(arg_keys[4], (EXPERTS, FF, D), FF ** -0.5, 0.21875, ((0, 8),))
    return {"tokens": tokens, "expert_ids": expert_ids, "gate_proj": gate_proj, "up_proj": up_proj, "down_proj": down_proj}


def expert_ffn(args):
    rows, gate_w, up_w, down_w = args
    gate_val = jnp.dot(rows, gate_w, preferred_element_type=jnp.float32)
    up_val = jnp.dot(rows, up_w, preferred_element_type=jnp.float32)
    hidden = (jax.nn.silu(gate_val) * up_val).astype(jnp.bfloat16)
    return jnp.dot(hidden, down_w, preferred_element_type=jnp.float32).astype(jnp.bfloat16)


def reference(tokens, expert_ids, gate_proj, up_proj, down_proj):
    choices = expert_ids[:, 0].astype(jnp.int32)
    onehot = (choices[:, None] == jnp.arange(EXPERTS, dtype=jnp.int32)[None, :]).astype(jnp.int32)
    before = jnp.cumsum(onehot, axis=0) - onehot
    slot_index = jnp.sum(before * onehot, axis=1).astype(jnp.int32)
    is_kept = slot_index < CAP
    buffer = jnp.zeros((EXPERTS, CAP, D), tokens.dtype)
    buffer = buffer.at[choices, slot_index].set(tokens, mode="drop")
    results = lax.map(expert_ffn, (buffer, gate_proj, up_proj, down_proj))
    picked = results[choices, jnp.minimum(slot_index, CAP - 1)]
    mixed = jnp.where(is_kept[:, None], picked, jnp.zeros_like(picked))
    return mixed, slot_index
```

```python
import functools

import jax
import jax.numpy as jnp
from jax import lax
from jax.experimental import pallas as pl
from jax.experimental.pallas import tpu as pltpu
from jax.sharding import PartitionSpec as P

MESH = pl.DeviceIdType.MESH
F32 = jnp.float32
BF16 = jnp.bfloat16
LANES = 128


def spread(step, n):
    half = (step // 2) * (2 * (step % 2) - 1)
    return jnp.where(step == 0, 0, n // 2 + half)


def kernel(
    n, dps, most, capacity,
    row_ids, col_ids, tok_ref, gate_hbm, up_hbm, down_hbm,
    out_ref, slot_ref,
    gate_ref, up_ref, down_ref, outgoing, arrived, results, returned,
    position, offset, counts, count_all, totals, total_all,
    weight_sem, go_send, go_recv, back_send, back_recv,
    count_send, count_recv, total_send, total_recv,
):
    me = lax.axis_index("expert")
    group = lax.axis_index("dp")
    tok = tok_ref.shape[0]
    width = tok_ref.shape[1]

    weights = [
        pltpu.make_async_copy(src.at[0], dst, weight_sem.at[i])
        for i, (src, dst) in enumerate(
            ((gate_hbm, gate_ref), (up_hbm, up_ref), (down_hbm, down_ref))
        )
    ]
    for copy in weights:
        copy.start()

    barrier = pltpu.get_barrier_semaphore()

    def greet(i, c):
        pl.semaphore_signal(
            barrier, inc=1, device_id={"expert": lax.rem(me + i, n)}, device_id_type=MESH
        )
        return c

    def greet_dp(i, c):
        pl.semaphore_signal(
            barrier, inc=1, device_id={"dp": lax.rem(group + i, dps)}, device_id_type=MESH
        )
        return c

    lax.fori_loop(1, n, greet, 0)
    lax.fori_loop(1, dps, greet_dp, 0)

    earlier = lax.broadcasted_iota(jnp.int32, (tok, tok), 0) < lax.broadcasted_iota(
        jnp.int32, (tok, tok), 1
    )
    later = lax.broadcasted_iota(jnp.int32, (tok, tok), 0) > lax.broadcasted_iota(
        jnp.int32, (tok, tok), 1
    )
    ids_row = row_ids[...]
    hot_row = (ids_row == lax.broadcasted_iota(jnp.int32, (n, tok), 0)).astype(F32)
    before_row = jnp.dot(
        hot_row.astype(BF16), earlier.astype(F32).astype(BF16), preferred_element_type=F32
    )
    rank_row = jnp.sum(before_row * hot_row, axis=0, keepdims=True).astype(jnp.int32)
    pos_row = ids_row * most + rank_row
    counts[...] = jnp.broadcast_to(
        jnp.sum(hot_row, axis=1, keepdims=True), (n, LANES)
    ).astype(jnp.int32)

    ids_col = col_ids[...]
    hot_col = (ids_col == lax.broadcasted_iota(jnp.int32, (tok, n), 1)).astype(F32)
    before_col = jnp.dot(
        later.astype(F32).astype(BF16), hot_col.astype(BF16), preferred_element_type=F32
    )
    rank_col = jnp.sum(before_col * hot_col, axis=1, keepdims=True).astype(jnp.int32)
    position[...] = ids_col * most + rank_col

    def go(dest, source):
        return pltpu.make_async_remote_copy(
            src_ref=outgoing.at[dest], dst_ref=arrived.at[source],
            send_sem=go_send.at[dest], recv_sem=go_recv.at[source],
            device_id={"expert": dest}, device_id_type=MESH,
        )

    def back(dest, source):
        return pltpu.make_async_remote_copy(
            src_ref=results.at[dest], dst_ref=returned.at[source],
            send_sem=back_send.at[dest], recv_sem=back_recv.at[source],
            device_id={"expert": dest}, device_id_type=MESH,
        )

    def count(dest, source):
        return pltpu.make_async_remote_copy(
            src_ref=counts, dst_ref=count_all.at[source],
            send_sem=count_send.at[dest], recv_sem=count_recv.at[source],
            device_id={"expert": dest}, device_id_type=MESH,
        )

    def total(dest, source):
        return pltpu.make_async_remote_copy(
            src_ref=totals, dst_ref=total_all.at[source],
            send_sem=total_send.at[dest], recv_sem=total_recv.at[source],
            device_id={"dp": dest}, device_id_type=MESH,
        )

    def pack(dest):
        pick = (
            lax.broadcasted_iota(jnp.int32, (most, tok), 0) + dest * most == pos_row
        ).astype(F32).astype(BF16)
        return jnp.dot(pick, tok_ref[...], preferred_element_type=F32).astype(BF16)

    pl.semaphore_wait(barrier, n + dps - 2)

    def dispatch(i, c):
        dest = lax.rem(me + spread(i, n), n)
        outgoing[dest] = pack(dest)
        go(dest, me).start()
        return c

    lax.fori_loop(1, n, dispatch, 0)

    def tell(i, c):
        count(lax.rem(me + i, n), me).start()
        return c

    lax.fori_loop(1, n, tell, 0)
    count_all[me] = counts[...]
    arrived[me] = pack(me)

    for copy in weights:
        copy.wait()

    def ffn(source):
        rows = arrived[source]
        gate = jnp.dot(rows, gate_ref[...], preferred_element_type=F32)
        up = jnp.dot(rows, up_ref[...], preferred_element_type=F32)
        hidden = (gate / (1.0 + jnp.exp(-gate)) * up).astype(BF16)
        return jnp.dot(hidden, down_ref[...], preferred_element_type=F32).astype(BF16)

    def expert_step(i, c):
        source = lax.rem(me + n - spread(i, n), n)

        @pl.when(i > 0)
        def _():
            go(me, source).wait_recv()

        results[source] = ffn(source)

        @pl.when(i > 0)
        def _():
            back(source, me).start()

        return c

    lax.fori_loop(0, n, expert_step, 0)

    def heard(i, c):
        count(me, lax.rem(me + i, n)).wait_recv()
        return c

    lax.fori_loop(1, n, heard, 0)

    def add(i, carry):
        inner, whole = carry
        here = count_all[i]
        return inner + here * (i < me).astype(jnp.int32), whole + here

    zero = jnp.zeros((n, LANES), jnp.int32)
    inner, whole = lax.fori_loop(0, n, add, (zero, zero))
    totals[...] = whole

    def tell_dp(i, c):
        total(lax.rem(group + i, dps), group).start()
        return c

    lax.fori_loop(1, dps, tell_dp, 0)
    total_all[group] = whole

    def heard_dp(i, c):
        total(group, lax.rem(group + i, dps)).wait_recv()
        return c

    lax.fori_loop(1, dps, heard_dp, 0)

    def add_dp(i, outer):
        return outer + total_all[i] * (i < group).astype(jnp.int32)

    offset[...] = inner + lax.fori_loop(0, dps, add_dp, zero)
    slot_ref[...] = (
        jnp.sum(
            hot_row * offset[:, 0:1].astype(F32), axis=0, keepdims=True
        ).astype(jnp.int32)
        + rank_row
    )

    piece = min(width, 512)

    def combine(source, block, first):
        lane = lax.broadcasted_iota(jnp.int32, (tok, most), 1)
        fits = offset[pl.ds(source, 1), 0:most] + lax.broadcasted_iota(
            jnp.int32, (1, most), 1
        ) < capacity
        pick = (lane + source * most == position[...]) & fits
        pick = pick.astype(F32).astype(BF16)
        for at in range(0, width, piece):
            part = jnp.dot(
                pick, block[source, :, at : at + piece], preferred_element_type=F32
            ).astype(BF16)
            if first:
                out_ref[:, at : at + piece] = part
            else:
                out_ref[:, at : at + piece] += part

    combine(me, results, True)

    def combine_step(i, c):
        source = lax.rem(me + n - spread(i, n), n)
        back(me, source).wait_recv()
        combine(source, returned, False)
        return c

    lax.fori_loop(1, n, combine_step, 0)

    def drain(i, c):
        other = lax.rem(me + i, n)
        go(other, me).wait_send()
        back(other, me).wait_send()
        count(other, me).wait_send()
        return c

    lax.fori_loop(1, n, drain, 0)

    def drain_dp(i, c):
        total(lax.rem(group + i, dps), group).wait_send()
        return c

    lax.fori_loop(1, dps, drain_dp, 0)


def on_device(tokens, expert_ids, gate_proj, up_proj, down_proj):
    tok, width = tokens.shape
    hidden = gate_proj.shape[2]
    n = lax.axis_size("expert")
    dps = lax.axis_size("dp")
    most = 2 * tok // n
    capacity = tok * dps
    vmem = pl.BlockSpec(memory_space=pltpu.VMEM)
    anywhere = pl.BlockSpec(memory_space=pltpu.MemorySpace.HBM)
    dma = pltpu.SemaphoreType.DMA
    block = pltpu.VMEM((n, most, width), BF16)
    mixed, slot = pl.pallas_call(
        functools.partial(kernel, n, dps, most, capacity),
        out_shape=(
            jax.ShapeDtypeStruct((tok, width), BF16),
            jax.ShapeDtypeStruct((1, tok), jnp.int32),
        ),
        in_specs=[vmem, vmem, vmem, anywhere, anywhere, anywhere],
        out_specs=(vmem, vmem),
        scratch_shapes=[
            pltpu.VMEM((width, hidden), BF16),
            pltpu.VMEM((width, hidden), BF16),
            pltpu.VMEM((hidden, width), BF16),
            block, block, block, block,
            pltpu.VMEM((tok, 1), jnp.int32),
            pltpu.VMEM((n, LANES), jnp.int32),
            pltpu.VMEM((n, LANES), jnp.int32),
            pltpu.VMEM((n, n, LANES), jnp.int32),
            pltpu.VMEM((n, LANES), jnp.int32),
            pltpu.VMEM((dps, n, LANES), jnp.int32),
            dma((3,)), dma((n,)), dma((n,)), dma((n,)), dma((n,)),
            dma((n,)), dma((n,)), dma((dps,)), dma((dps,)),
        ],
        compiler_params=pltpu.CompilerParams(
            collective_id=0, has_side_effects=True, vmem_limit_bytes=60 * 2**20
        ),
    )(
        expert_ids.reshape(1, tok), expert_ids, tokens, gate_proj, up_proj, down_proj
    )
    return mixed, slot.reshape(tok)


def solution(mesh):
    in_specs = (
        P(("dp", "expert"), None),
        P(("dp", "expert"), None),
        P("expert", None, None),
        P("expert", None, None),
        P("expert", None, None),
    )
    out_specs = (P(("dp", "expert"), None), P(("dp", "expert")))
    return jax.shard_map(
        on_device, mesh=mesh, in_specs=in_specs, out_specs=out_specs, check_vma=False
    )
```

```python
import functools

import jax
import jax.numpy as jnp
from jax import lax
from jax.experimental import pallas as pl
from jax.experimental.pallas import tpu as pltpu
from jax.sharding import PartitionSpec as P

MESH = pl.DeviceIdType.MESH
F32 = jnp.float32
BF16 = jnp.bfloat16
LANES = 128


def spread(step, n):
    half = (step // 2) * (2 * (step % 2) - 1)
    return jnp.where(step == 0, 0, n // 2 + half)


def direct_kernel(
    n, dps, most, capacity,
    row_ids, col_ids, tok_ref, gate_hbm, up_hbm, down_hbm,
    out_ref, slot_ref,
    gate_ref, up_ref, down_ref, outgoing, arrived, results, returned,
    position, offset, counts, count_all, totals, total_all,
    weight_sem, go_send, go_recv, back_send, back_recv,
    count_send, count_recv, total_send, total_recv,
):
    me = lax.axis_index("expert")
    group = lax.axis_index("dp")
    tok = tok_ref.shape[0]
    width = tok_ref.shape[1]

    weights = [
        pltpu.make_async_copy(src.at[0], dst, weight_sem.at[i])
        for i, (src, dst) in enumerate(
            ((gate_hbm, gate_ref), (up_hbm, up_ref), (down_hbm, down_ref))
        )
    ]
    for copy in weights:
        copy.start()

    barrier = pltpu.get_barrier_semaphore()

    def greet(i, c):
        pl.semaphore_signal(
            barrier, inc=1, device_id={"expert": lax.rem(me + i, n)}, device_id_type=MESH
        )
        return c

    def greet_dp(i, c):
        pl.semaphore_signal(
            barrier, inc=1, device_id={"dp": lax.rem(group + i, dps)}, device_id_type=MESH
        )
        return c

    lax.fori_loop(1, n, greet, 0)
    lax.fori_loop(1, dps, greet_dp, 0)

    earlier = lax.broadcasted_iota(jnp.int32, (tok, tok), 0) < lax.broadcasted_iota(
        jnp.int32, (tok, tok), 1
    )
    later = lax.broadcasted_iota(jnp.int32, (tok, tok), 0) > lax.broadcasted_iota(
        jnp.int32, (tok, tok), 1
    )
    ids_row = row_ids[...]
    hot_row = (ids_row == lax.broadcasted_iota(jnp.int32, (n, tok), 0)).astype(F32)
    before_row = jnp.dot(
        hot_row.astype(BF16), earlier.astype(F32).astype(BF16), preferred_element_type=F32
    )
    rank_row = jnp.sum(before_row * hot_row, axis=0, keepdims=True).astype(jnp.int32)
    pos_row = ids_row * most + rank_row
    counts[...] = jnp.broadcast_to(
        jnp.sum(hot_row, axis=1, keepdims=True), (n, LANES)
    ).astype(jnp.int32)

    ids_col = col_ids[...]
    hot_col = (ids_col == lax.broadcasted_iota(jnp.int32, (tok, n), 1)).astype(F32)
    before_col = jnp.dot(
        later.astype(F32).astype(BF16), hot_col.astype(BF16), preferred_element_type=F32
    )
    rank_col = jnp.sum(before_col * hot_col, axis=1, keepdims=True).astype(jnp.int32)
    position[...] = ids_col * most + rank_col

    def go(dest, source):
        return pltpu.make_async_remote_copy(
            src_ref=outgoing.at[dest], dst_ref=arrived.at[source],
            send_sem=go_send.at[dest], recv_sem=go_recv.at[source],
            device_id={"expert": dest}, device_id_type=MESH,
        )

    def back(dest, source):
        return pltpu.make_async_remote_copy(
            src_ref=results.at[dest], dst_ref=returned.at[source],
            send_sem=back_send.at[dest], recv_sem=back_recv.at[source],
            device_id={"expert": dest}, device_id_type=MESH,
        )

    def count(dest, source):
        return pltpu.make_async_remote_copy(
            src_ref=counts, dst_ref=count_all.at[source],
            send_sem=count_send.at[dest], recv_sem=count_recv.at[source],
            device_id={"expert": dest}, device_id_type=MESH,
        )

    def total(dest, source):
        return pltpu.make_async_remote_copy(
            src_ref=totals, dst_ref=total_all.at[source],
            send_sem=total_send.at[dest], recv_sem=total_recv.at[source],
            device_id={"dp": dest}, device_id_type=MESH,
        )

    def pack(dest):
        pick = (
            lax.broadcasted_iota(jnp.int32, (most, tok), 0) + dest * most == pos_row
        ).astype(F32).astype(BF16)
        return jnp.dot(pick, tok_ref[...], preferred_element_type=F32).astype(BF16)

    pl.semaphore_wait(barrier, n + dps - 2)

    def dispatch(i, c):
        dest = lax.rem(me + spread(i, n), n)
        outgoing[dest] = pack(dest)
        go(dest, me).start()
        return c

    lax.fori_loop(1, n, dispatch, 0)

    def tell(i, c):
        count(lax.rem(me + i, n), me).start()
        return c

    lax.fori_loop(1, n, tell, 0)
    count_all[me] = counts[...]
    arrived[me] = pack(me)

    for copy in weights:
        copy.wait()

    def ffn(source):
        rows = arrived[source]
        gate = jnp.dot(rows, gate_ref[...], preferred_element_type=F32)
        up = jnp.dot(rows, up_ref[...], preferred_element_type=F32)
        hidden = (gate / (1.0 + jnp.exp(-gate)) * up).astype(BF16)
        return jnp.dot(hidden, down_ref[...], preferred_element_type=F32).astype(BF16)

    def expert_step(i, c):
        source = lax.rem(me + n - spread(i, n), n)

        @pl.when(i > 0)
        def _():
            go(me, source).wait_recv()

        results[source] = ffn(source)

        @pl.when(i > 0)
        def _():
            back(source, me).start()

        return c

    lax.fori_loop(0, n, expert_step, 0)

    def heard(i, c):
        count(me, lax.rem(me + i, n)).wait_recv()
        return c

    lax.fori_loop(1, n, heard, 0)

    def add(i, carry):
        inner, whole = carry
        here = count_all[i]
        return inner + here * (i < me).astype(jnp.int32), whole + here

    zero = jnp.zeros((n, LANES), jnp.int32)
    inner, whole = lax.fori_loop(0, n, add, (zero, zero))
    totals[...] = whole

    def tell_dp(i, c):
        total(lax.rem(group + i, dps), group).start()
        return c

    lax.fori_loop(1, dps, tell_dp, 0)
    total_all[group] = whole

    def heard_dp(i, c):
        total(group, lax.rem(group + i, dps)).wait_recv()
        return c

    lax.fori_loop(1, dps, heard_dp, 0)

    def add_dp(i, outer):
        return outer + total_all[i] * (i < group).astype(jnp.int32)

    offset[...] = inner + lax.fori_loop(0, dps, add_dp, zero)
    slot_ref[...] = (
        jnp.sum(
            hot_row * offset[:, 0:1].astype(F32), axis=0, keepdims=True
        ).astype(jnp.int32)
        + rank_row
    )

    piece = min(width, 512)

    def combine(source, block, first):
        lane = lax.broadcasted_iota(jnp.int32, (tok, most), 1)
        fits = offset[pl.ds(source, 1), 0:most] + lax.broadcasted_iota(
            jnp.int32, (1, most), 1
        ) < capacity
        pick = (lane + source * most == position[...]) & fits
        pick = pick.astype(F32).astype(BF16)
        for at in range(0, width, piece):
            part = jnp.dot(
                pick, block[source, :, at : at + piece], preferred_element_type=F32
            ).astype(BF16)
            if first:
                out_ref[:, at : at + piece] = part
            else:
                out_ref[:, at : at + piece] += part

    combine(me, results, True)

    def combine_step(i, c):
        source = lax.rem(me + n - spread(i, n), n)
        back(me, source).wait_recv()
        combine(source, returned, False)
        return c

    lax.fori_loop(1, n, combine_step, 0)

    def drain(i, c):
        other = lax.rem(me + i, n)
        go(other, me).wait_send()
        back(other, me).wait_send()
        count(other, me).wait_send()
        return c

    lax.fori_loop(1, n, drain, 0)

    def drain_dp(i, c):
        total(lax.rem(group + i, dps), group).wait_send()
        return c

    lax.fori_loop(1, dps, drain_dp, 0)


def direct(tokens, expert_ids, gate_proj, up_proj, down_proj):
    tok, width = tokens.shape
    hidden = gate_proj.shape[2]
    n = lax.axis_size("expert")
    dps = lax.axis_size("dp")
    most = 2 * tok // n
    capacity = tok * dps
    vmem = pl.BlockSpec(memory_space=pltpu.VMEM)
    anywhere = pl.BlockSpec(memory_space=pltpu.MemorySpace.HBM)
    dma = pltpu.SemaphoreType.DMA
    block = pltpu.VMEM((n, most, width), BF16)
    mixed, slot = pl.pallas_call(
        functools.partial(direct_kernel, n, dps, most, capacity),
        out_shape=(
            jax.ShapeDtypeStruct((tok, width), BF16),
            jax.ShapeDtypeStruct((1, tok), jnp.int32),
        ),
        in_specs=[vmem, vmem, vmem, anywhere, anywhere, anywhere],
        out_specs=(vmem, vmem),
        scratch_shapes=[
            pltpu.VMEM((width, hidden), BF16),
            pltpu.VMEM((width, hidden), BF16),
            pltpu.VMEM((hidden, width), BF16),
            block, block, block, block,
            pltpu.VMEM((tok, 1), jnp.int32),
            pltpu.VMEM((n, LANES), jnp.int32),
            pltpu.VMEM((n, LANES), jnp.int32),
            pltpu.VMEM((n, n, LANES), jnp.int32),
            pltpu.VMEM((n, LANES), jnp.int32),
            pltpu.VMEM((dps, n, LANES), jnp.int32),
            dma((3,)), dma((n,)), dma((n,)), dma((n,)), dma((n,)),
            dma((n,)), dma((n,)), dma((dps,)), dma((dps,)),
        ],
        compiler_params=pltpu.CompilerParams(
            collective_id=0, has_side_effects=True, vmem_limit_bytes=60 * 2**20
        ),
    )(
        expert_ids.reshape(1, tok), expert_ids, tokens, gate_proj, up_proj, down_proj
    )
    return mixed, slot.reshape(tok)


def entering(part, axis, combine, identity):
    place = lax.axis_index(axis)
    gathered = lax.all_gather(part, axis)
    state = jnp.zeros_like(part) + jnp.asarray(identity, part.dtype)

    def one(hop, state):
        return combine(state, lax.dynamic_index_in_dim(gathered, hop, 0, False))

    return lax.fori_loop(0, place, one, state)


def add_counts(earlier, later):
    return earlier + later


def expert_ffn(rows, gate_proj, up_proj, down_proj):
    gate_val = jnp.dot(rows, gate_proj[0], preferred_element_type=jnp.float32)
    up_val = jnp.dot(rows, up_proj[0], preferred_element_type=jnp.float32)
    hidden = (jax.nn.silu(gate_val) * up_val).astype(jnp.bfloat16)
    return jnp.dot(hidden, down_proj[0], preferred_element_type=jnp.float32).astype(jnp.bfloat16)


def padded(tokens, expert_ids, gate_proj, up_proj, down_proj):
    tok_rows, width = tokens.shape
    experts_all = lax.axis_size("expert")
    most = 2 * tok_rows // experts_all
    capacity = tok_rows * lax.axis_size("dp")
    choices = expert_ids[:, 0]
    onehot = (choices[:, None] == jnp.arange(experts_all, dtype=jnp.int32)[None, :]).astype(
        jnp.int32
    )
    counts = jnp.sum(onehot, axis=0)
    inner = entering(counts, "expert", add_counts, jnp.zeros_like(counts))
    totals = lax.psum(counts, "expert")
    outer = entering(totals, "dp", add_counts, jnp.zeros_like(totals))
    offset = inner + outer
    before = jnp.cumsum(onehot, axis=0) - onehot
    local_rank = jnp.sum(before * onehot, axis=1)
    global_slot = (jnp.sum(onehot * offset[None, :], axis=1) + local_rank).astype(jnp.int32)
    is_kept = global_slot < capacity
    position = choices * most + local_rank
    targets = jnp.arange(experts_all * most, dtype=jnp.int32)
    dispatch = ((targets[:, None] == position[None, :]) & is_kept[None, :]).astype(jnp.bfloat16)
    outgoing = jnp.dot(dispatch, tokens, preferred_element_type=jnp.float32).astype(jnp.bfloat16)
    outgoing = outgoing.reshape(experts_all, most, width)
    arrived = lax.all_to_all(outgoing, "expert", split_axis=0, concat_axis=0, tiled=True)
    sources, slots_here, _ = arrived.shape
    flat = arrived.reshape(sources * slots_here, width)
    returned = lax.all_to_all(
        expert_ffn(flat, gate_proj, up_proj, down_proj).reshape(sources, slots_here, width),
        "expert",
        split_axis=0,
        concat_axis=0,
        tiled=True,
    )
    flat_back = returned.reshape(experts_all * most, width)
    mixed = lax.dot_general(
        dispatch, flat_back, (((0,), (0,)), ((), ())), preferred_element_type=jnp.float32
    )
    return (mixed.astype(jnp.bfloat16), global_slot)


def relay_kernel(
    n, dps, most, base, dense, capacity,
    row_ids, col_ids, tok_ref, gate_hbm, up_hbm, down_hbm,
    out_ref, slot_ref, flag_ref,
    gate_ref, up_ref, down_ref, outgoing, arrived, results, returned,
    x_out, x_in, x_back, x_home, relay_out, relay_in,
    position, x_position, offset, x_first, x_size, r_first, r_size,
    counts, count_all, totals, total_all,
    weight_sem, go_send, go_recv, back_send, back_recv,
    over_send, over_recv, gather_send, gather_recv, x_send, x_recv,
    count_send, count_recv, total_send, total_recv,
):
    me = lax.axis_index("expert")
    group = lax.axis_index("dp")
    tok, width = tok_ref.shape
    hn = n // 2
    over = most - base
    near = lax.div(me, hn) * hn
    far = hn - near
    place = me - near
    partner = far + place
    piece = min(width, 512)

    def around(i):
        return lax.rem(place + i, hn)

    weights = [
        pltpu.make_async_copy(src.at[0], dst, weight_sem.at[i])
        for i, (src, dst) in enumerate(
            ((gate_hbm, gate_ref), (up_hbm, up_ref), (down_hbm, down_ref))
        )
    ]
    for copy in weights:
        copy.start()

    barrier = pltpu.get_barrier_semaphore()

    def greet(i, c):
        pl.semaphore_signal(
            barrier, inc=1, device_id={"expert": lax.rem(me + i, n)}, device_id_type=MESH
        )
        return c

    def greet_dp(i, c):
        pl.semaphore_signal(
            barrier, inc=1, device_id={"dp": lax.rem(group + i, dps)}, device_id_type=MESH
        )
        return c

    lax.fori_loop(1, n, greet, 0)
    lax.fori_loop(1, dps, greet_dp, 0)

    def iota(shape, axis):
        return lax.broadcasted_iota(jnp.int32, shape, axis)

    def ones(mask):
        return mask.astype(F32).astype(BF16)

    def dot(a, b):
        return jnp.dot(a, b, preferred_element_type=F32)

    def excess(count, half):
        rows = iota((n, LANES), 0)
        inside = (rows >= half) & (rows < half + hn)
        size = jnp.where(inside, jnp.maximum(count - base, 0), 0)
        first = dot(
            ones(iota((n, n), 1) < iota((n, n), 0)), size.astype(F32).astype(BF16)
        ).astype(jnp.int32)
        return first, size

    ids_row = row_ids[...]
    hot_row = (ids_row == iota((n, tok), 0)).astype(F32)
    before_row = dot(hot_row.astype(BF16), ones(iota((tok, tok), 0) < iota((tok, tok), 1)))
    rank_row = jnp.sum(before_row * hot_row, axis=0, keepdims=True).astype(jnp.int32)
    pos_row = ids_row * most + rank_row
    mine = jnp.broadcast_to(
        jnp.sum(hot_row, axis=1, keepdims=True), (n, LANES)
    ).astype(jnp.int32)
    counts[...] = mine
    first, size = excess(mine, far)
    x_first[...] = first
    x_size[...] = size
    start_row = jnp.sum(
        hot_row * x_first[:, 0:1].astype(F32), axis=0, keepdims=True
    ).astype(jnp.int32)
    x_row = jnp.where(
        (ids_row >= far) & (ids_row < far + hn) & (rank_row >= base),
        start_row + rank_row - base, -1,
    )

    ids_col = col_ids[...]
    hot_col = (ids_col == iota((tok, n), 1)).astype(F32)

    def go(dest, source, far_off):
        rows = pl.ds(0, base if far_off else most)
        return pltpu.make_async_remote_copy(
            src_ref=outgoing.at[dest, rows], dst_ref=arrived.at[source, rows],
            send_sem=go_send.at[dest], recv_sem=go_recv.at[source],
            device_id={"expert": dest}, device_id_type=MESH,
        )

    def back(dest, source, far_off):
        rows = pl.ds(0, base if far_off else most)
        return pltpu.make_async_remote_copy(
            src_ref=results.at[dest, rows], dst_ref=returned.at[source, rows],
            send_sem=back_send.at[dest], recv_sem=back_recv.at[source],
            device_id={"expert": dest}, device_id_type=MESH,
        )

    def forward(dest, slot, source):
        return pltpu.make_async_remote_copy(
            src_ref=relay_out.at[slot], dst_ref=arrived.at[source, pl.ds(base, over)],
            send_sem=over_send.at[slot], recv_sem=over_recv.at[source],
            device_id={"expert": dest}, device_id_type=MESH,
        )

    def gather(dest, source, slot):
        return pltpu.make_async_remote_copy(
            src_ref=results.at[source, pl.ds(base, over)], dst_ref=relay_in.at[slot],
            send_sem=gather_send.at[source], recv_sem=gather_recv.at[slot],
            device_id={"expert": dest}, device_id_type=MESH,
        )

    def cross(which, src, dst):
        return pltpu.make_async_remote_copy(
            src_ref=src, dst_ref=dst,
            send_sem=x_send.at[which], recv_sem=x_recv.at[which],
            device_id={"expert": partner}, device_id_type=MESH,
        )

    def count(dest, source):
        return pltpu.make_async_remote_copy(
            src_ref=counts, dst_ref=count_all.at[source],
            send_sem=count_send.at[dest], recv_sem=count_recv.at[source],
            device_id={"expert": dest}, device_id_type=MESH,
        )

    def total(dest, source):
        return pltpu.make_async_remote_copy(
            src_ref=totals, dst_ref=total_all.at[source],
            send_sem=total_send.at[dest], recv_sem=total_recv.at[source],
            device_id={"dp": dest}, device_id_type=MESH,
        )

    def pack(dest, rows):
        pick = ones(iota((rows, tok), 0) + dest * most == pos_row)
        return dot(pick, tok_ref[...]).astype(BF16)

    x_out[...] = dot(ones(iota((dense, tok), 0) == x_row), tok_ref[...]).astype(BF16)

    pl.semaphore_wait(barrier, n + dps - 2)

    def tell(i, c):
        count(lax.rem(me + i, n), me).start()
        return c

    lax.fori_loop(1, n, tell, 0)
    send_x = cross(0, x_out, x_in)
    send_x.start()

    def dispatch_near(i, c):
        dest = near + around(i)
        outgoing[dest] = pack(dest, most)
        go(dest, me, False).start()
        return c

    lax.fori_loop(1, hn, dispatch_near, 0)

    def dispatch_far(i, c):
        dest = far + around(i)
        outgoing[dest, pl.ds(0, base)] = pack(dest, base)
        go(dest, me, True).start()
        return c

    lax.fori_loop(0, hn, dispatch_far, 0)
    count_all[me] = mine
    arrived[me] = pack(me, most)

    before_col = dot(ones(iota((tok, tok), 0) > iota((tok, tok), 1)), hot_col.astype(BF16))
    rank_col = jnp.sum(before_col * hot_col, axis=1, keepdims=True).astype(jnp.int32)
    position[...] = ids_col * most + rank_col
    lane = iota((1, n), 1)
    size_lane = jnp.where(
        (lane >= far) & (lane < far + hn),
        jnp.maximum(jnp.sum(hot_col, axis=0, keepdims=True) - base, 0.0), 0.0,
    )
    first_lane = dot(
        jnp.broadcast_to(size_lane, (16, n)).astype(BF16),
        ones(iota((n, n), 0) < iota((n, n), 1)),
    )[0:1]
    start_col = jnp.sum(hot_col * first_lane, axis=1, keepdims=True).astype(jnp.int32)
    x_position[...] = jnp.where(
        (ids_col >= far) & (ids_col < far + hn) & (rank_col >= base),
        start_col + rank_col - base, -1,
    )

    for copy in weights:
        copy.wait()

    def ffn(source):
        rows = arrived[source]
        gate = dot(rows, gate_ref[...])
        up = dot(rows, up_ref[...])
        hidden = (gate / (1.0 + jnp.exp(-gate)) * up).astype(BF16)
        results[source] = dot(hidden, down_ref[...]).astype(BF16)

    def near_step(i, c):
        source = near + lax.rem(place + hn - i, hn)

        @pl.when(i > 0)
        def _():
            go(me, source, False).wait_recv()

        ffn(source)

        @pl.when(i > 0)
        def _():
            back(source, me, False).start()

        @pl.when(i == 0)
        def _():
            unpack()

        return c

    def unpack():
        count(me, partner).wait_recv()
        send_x.wait_recv()
        first, size = excess(count_all[partner], near)
        r_first[...] = first
        r_size[...] = size

        def one(i, c):
            slot = around(i)
            dest = near + slot
            row = iota((over, dense), 0)
            pick = (iota((over, dense), 1) == row + r_first[pl.ds(dest, 1), 0:1]) & (
                row < r_size[pl.ds(dest, 1), 0:1]
            )
            block = dot(ones(pick), x_in[...]).astype(BF16)

            @pl.when(i == 0)
            def _():
                arrived[partner, pl.ds(base, over)] = block

            @pl.when(i > 0)
            def _():
                relay_out[slot] = block
                forward(dest, slot, partner).start()

            return c

        lax.fori_loop(0, hn, one, 0)

    lax.fori_loop(0, hn, near_step, 0)

    def far_step(i, c):
        slot = lax.rem(place + hn - i, hn)
        source = far + slot
        go(me, source, True).wait_recv()

        @pl.when(i > 0)
        def _():
            forward(me, place, source).wait_recv()

        ffn(source)
        back(source, me, True).start()

        @pl.when(i > 0)
        def _():
            gather(near + slot, source, place).start()

        @pl.when(i == 0)
        def _():
            relay_in[place] = results[source, pl.ds(base, over)]

        return c

    lax.fori_loop(0, hn, far_step, 0)

    def collect(i, c):
        gather(me, partner, around(i)).wait_recv()
        return c

    lax.fori_loop(1, hn, collect, 0)
    picks = []
    for slot in range(hn):
        column = iota((dense, over), 1)
        pick = (
            iota((dense, over), 0) == column + r_first[pl.ds(near + slot, 1), 0:1]
        ) & (column < r_size[pl.ds(near + slot, 1), 0:1])
        picks.append(ones(pick))
    for at in range(0, width, piece):
        acc = dot(picks[0], relay_in[0, :, at : at + piece])
        for slot in range(1, hn):
            acc += dot(picks[slot], relay_in[slot, :, at : at + piece])
        x_back[:, at : at + piece] = acc.astype(BF16)
    send_back = cross(1, x_back, x_home)
    send_back.start()

    def heard(i, c):
        @pl.when(i != hn)
        def _():
            count(me, lax.rem(me + i, n)).wait_recv()

        return c

    lax.fori_loop(1, n, heard, 0)

    def add(i, carry):
        inner, whole, need = carry
        here = count_all[i]
        other = hn - lax.div(i, hn) * hn
        rows = iota((n, LANES), 0)
        outside = (rows >= other) & (rows < other + hn)
        extra = jnp.sum(
            jnp.where(outside, jnp.maximum(here - base, 0), 0), axis=0, keepdims=True
        )
        return (
            inner + here * (i < me).astype(jnp.int32), whole + here, jnp.maximum(need, extra)
        )

    zero = jnp.zeros((n, LANES), jnp.int32)
    inner, whole, need = lax.fori_loop(
        0, n, add, (zero, zero, jnp.zeros((1, LANES), jnp.int32))
    )
    need = jnp.broadcast_to(need, (8, LANES))
    totals[0] = whole
    totals[1] = need

    def tell_dp(i, c):
        total(lax.rem(group + i, dps), group).start()
        return c

    lax.fori_loop(1, dps, tell_dp, 0)
    total_all[group, 0] = whole
    total_all[group, 1] = need

    def heard_dp(i, c):
        total(group, lax.rem(group + i, dps)).wait_recv()
        return c

    lax.fori_loop(1, dps, heard_dp, 0)

    def add_dp(i, carry):
        outer, most_needed = carry
        return (
            outer + total_all[i, 0] * (i < group).astype(jnp.int32),
            jnp.maximum(most_needed, total_all[i, 1]),
        )

    outer, needed = lax.fori_loop(0, dps, add_dp, (zero, need))
    offset[...] = inner + outer
    flag_ref[...] = (needed > dense).astype(jnp.int32)
    slot_ref[...] = (
        jnp.sum(hot_row * offset[:, 0:1].astype(F32), axis=0, keepdims=True).astype(jnp.int32)
        + rank_row
    )

    def combine(pick, block, first):
        for at in range(0, width, piece):
            part = dot(pick, block[:, at : at + piece]).astype(BF16)
            if first:
                out_ref[:, at : at + piece] = part
            else:
                out_ref[:, at : at + piece] += part

    def choose(source, rows):
        fits = offset[pl.ds(source, 1), 0:rows] + iota((1, rows), 1) < capacity
        return ones((iota((tok, rows), 1) + source * most == position[...]) & fits)

    combine(choose(me, most), results.at[me], True)

    def near_back(i, c):
        source = near + lax.rem(place + hn - i, hn)
        back(me, source, False).wait_recv()
        combine(choose(source, most), returned.at[source], False)
        return c

    lax.fori_loop(1, hn, near_back, 0)

    def far_back(i, c):
        source = far + lax.rem(place + hn - i, hn)
        back(me, source, True).wait_recv()
        combine(choose(source, base), returned.at[source, pl.ds(0, base)], False)
        return c

    lax.fori_loop(0, hn, far_back, 0)

    entry = iota((1, dense), 1)
    keep = jnp.zeros((1, dense), jnp.int32)
    for slot in range(hn):
        row = pl.ds(far + slot, 1)
        rank = entry - x_first[row, 0:1]
        inside = (rank >= 0) & (rank < x_size[row, 0:1])
        keep += (inside & (offset[row, 0:1] + rank + base < capacity)).astype(jnp.int32)
    send_back.wait_recv()
    combine(
        ones((iota((tok, dense), 1) == x_position[...]) & (keep > 0)), x_home, False
    )

    send_x.wait_send()
    send_back.wait_send()

    def drain_near(i, c):
        slot = around(i)
        other = near + slot
        go(other, me, False).wait_send()
        back(other, me, False).wait_send()
        forward(other, slot, partner).wait_send()
        gather(other, far + slot, place).wait_send()
        return c

    lax.fori_loop(1, hn, drain_near, 0)

    def drain_far(i, c):
        other = far + i
        go(other, me, True).wait_send()
        back(other, me, True).wait_send()
        return c

    lax.fori_loop(0, hn, drain_far, 0)

    def drain(i, c):
        count(lax.rem(me + i, n), me).wait_send()
        return c

    lax.fori_loop(1, n, drain, 0)

    def drain_dp(i, c):
        total(lax.rem(group + i, dps), group).wait_send()
        return c

    lax.fori_loop(1, dps, drain_dp, 0)


def relayed(tokens, expert_ids, gate_proj, up_proj, down_proj):
    tok, width = tokens.shape
    hidden = gate_proj.shape[2]
    n = lax.axis_size("expert")
    dps = lax.axis_size("dp")
    most = 2 * tok // n
    base = most // 2
    over = most - base
    dense = 5 * most // 4
    capacity = tok * dps
    vmem = pl.BlockSpec(memory_space=pltpu.VMEM)
    anywhere = pl.BlockSpec(memory_space=pltpu.MemorySpace.HBM)
    dma = pltpu.SemaphoreType.DMA
    block = pltpu.VMEM((n, most, width), BF16)
    packed = pltpu.VMEM((dense, width), BF16)
    relay = pltpu.VMEM((n // 2, over, width), BF16)
    table = pltpu.VMEM((n, LANES), jnp.int32)
    column = pltpu.VMEM((tok, 1), jnp.int32)
    mixed, slot, flag = pl.pallas_call(
        functools.partial(relay_kernel, n, dps, most, base, dense, capacity),
        out_shape=(
            jax.ShapeDtypeStruct((tok, width), BF16),
            jax.ShapeDtypeStruct((1, tok), jnp.int32),
            jax.ShapeDtypeStruct((8, LANES), jnp.int32),
        ),
        in_specs=[vmem, vmem, vmem, anywhere, anywhere, anywhere],
        out_specs=(vmem, vmem, vmem),
        scratch_shapes=[
            pltpu.VMEM((width, hidden), BF16),
            pltpu.VMEM((width, hidden), BF16),
            pltpu.VMEM((hidden, width), BF16),
            block, block, block, block,
            packed, packed, packed, packed, relay, relay,
            column, column, table, table, table, table, table,
            table,
            pltpu.VMEM((n, n, LANES), jnp.int32),
            pltpu.VMEM((2, n, LANES), jnp.int32),
            pltpu.VMEM((dps, 2, n, LANES), jnp.int32),
            dma((3,)), dma((n,)), dma((n,)), dma((n,)), dma((n,)),
            dma((n // 2,)), dma((n,)), dma((n,)), dma((n // 2,)), dma((2,)), dma((2,)),
            dma((n,)), dma((n,)), dma((dps,)), dma((dps,)),
        ],
        compiler_params=pltpu.CompilerParams(
            collective_id=0, has_side_effects=True, vmem_limit_bytes=60 * 2**20
        ),
    )(
        expert_ids.reshape(1, tok), expert_ids, tokens, gate_proj, up_proj, down_proj
    )
    return lax.cond(
        flag[0, 0] > 0,
        lambda: padded(tokens, expert_ids, gate_proj, up_proj, down_proj),
        lambda: (mixed, slot.reshape(tok)),
    )


def on_device(tokens, expert_ids, gate_proj, up_proj, down_proj):
    n = lax.axis_size("expert")
    if n == 8 and tokens.shape[0] // n % 16 == 0:
        return relayed(tokens, expert_ids, gate_proj, up_proj, down_proj)
    return direct(tokens, expert_ids, gate_proj, up_proj, down_proj)


def solution(mesh):
    in_specs = (
        P(("dp", "expert"), None),
        P(("dp", "expert"), None),
        P("expert", None, None),
        P("expert", None, None),
        P("expert", None, None),
    )
    out_specs = (P(("dp", "expert"), None), P(("dp", "expert")))
    return jax.shard_map(
        on_device, mesh=mesh, in_specs=in_specs, out_specs=out_specs, check_vma=False
    )
```

```python
import functools

import jax
import jax.numpy as jnp
from jax import lax
from jax.experimental import pallas as pl
from jax.experimental.pallas import tpu as pltpu
from jax.sharding import PartitionSpec as P

MESH = pl.DeviceIdType.MESH
F32 = jnp.float32
BF16 = jnp.bfloat16
LANES = 128


def spread(step, n):
    half = (step // 2) * (2 * (step % 2) - 1)
    return jnp.where(step == 0, 0, n // 2 + half)


def direct_kernel(
    n, dps, most, capacity,
    row_ids, col_ids, tok_ref, gate_hbm, up_hbm, down_hbm,
    out_ref, slot_ref,
    gate_ref, up_ref, down_ref, outgoing, arrived, results, returned,
    position, offset, counts, count_all, totals, total_all,
    weight_sem, go_send, go_recv, back_send, back_recv,
    count_send, count_recv, total_send, total_recv,
):
    me = lax.axis_index("expert")
    group = lax.axis_index("dp")
    tok = tok_ref.shape[0]
    width = tok_ref.shape[1]

    weights = [
        pltpu.make_async_copy(src.at[0], dst, weight_sem.at[i])
        for i, (src, dst) in enumerate(
            ((gate_hbm, gate_ref), (up_hbm, up_ref), (down_hbm, down_ref))
        )
    ]
    for copy in weights:
        copy.start()

    barrier = pltpu.get_barrier_semaphore()

    def greet(i, c):
        pl.semaphore_signal(
            barrier, inc=1, device_id={"expert": lax.rem(me + i, n)}, device_id_type=MESH
        )
        return c

    def greet_dp(i, c):
        pl.semaphore_signal(
            barrier, inc=1, device_id={"dp": lax.rem(group + i, dps)}, device_id_type=MESH
        )
        return c

    lax.fori_loop(1, n, greet, 0)
    lax.fori_loop(1, dps, greet_dp, 0)

    earlier = lax.broadcasted_iota(jnp.int32, (tok, tok), 0) < lax.broadcasted_iota(
        jnp.int32, (tok, tok), 1
    )
    later = lax.broadcasted_iota(jnp.int32, (tok, tok), 0) > lax.broadcasted_iota(
        jnp.int32, (tok, tok), 1
    )
    ids_row = row_ids[...]
    hot_row = (ids_row == lax.broadcasted_iota(jnp.int32, (n, tok), 0)).astype(F32)
    before_row = jnp.dot(
        hot_row.astype(BF16), earlier.astype(F32).astype(BF16), preferred_element_type=F32
    )
    rank_row = jnp.sum(before_row * hot_row, axis=0, keepdims=True).astype(jnp.int32)
    pos_row = ids_row * most + rank_row
    counts[...] = jnp.broadcast_to(
        jnp.sum(hot_row, axis=1, keepdims=True), (n, LANES)
    ).astype(jnp.int32)

    ids_col = col_ids[...]
    hot_col = (ids_col == lax.broadcasted_iota(jnp.int32, (tok, n), 1)).astype(F32)
    before_col = jnp.dot(
        later.astype(F32).astype(BF16), hot_col.astype(BF16), preferred_element_type=F32
    )
    rank_col = jnp.sum(before_col * hot_col, axis=1, keepdims=True).astype(jnp.int32)
    position[...] = ids_col * most + rank_col

    def go(dest, source):
        return pltpu.make_async_remote_copy(
            src_ref=outgoing.at[dest], dst_ref=arrived.at[source],
            send_sem=go_send.at[dest], recv_sem=go_recv.at[source],
            device_id={"expert": dest}, device_id_type=MESH,
        )

    def back(dest, source):
        return pltpu.make_async_remote_copy(
            src_ref=results.at[dest], dst_ref=returned.at[source],
            send_sem=back_send.at[dest], recv_sem=back_recv.at[source],
            device_id={"expert": dest}, device_id_type=MESH,
        )

    def count(dest, source):
        return pltpu.make_async_remote_copy(
            src_ref=counts, dst_ref=count_all.at[source],
            send_sem=count_send.at[dest], recv_sem=count_recv.at[source],
            device_id={"expert": dest}, device_id_type=MESH,
        )

    def total(dest, source):
        return pltpu.make_async_remote_copy(
            src_ref=totals, dst_ref=total_all.at[source],
            send_sem=total_send.at[dest], recv_sem=total_recv.at[source],
            device_id={"dp": dest}, device_id_type=MESH,
        )

    def pack(dest):
        pick = (
            lax.broadcasted_iota(jnp.int32, (most, tok), 0) + dest * most == pos_row
        ).astype(F32).astype(BF16)
        return jnp.dot(pick, tok_ref[...], preferred_element_type=F32).astype(BF16)

    pl.semaphore_wait(barrier, n + dps - 2)

    def dispatch(i, c):
        dest = lax.rem(me + spread(i, n), n)
        outgoing[dest] = pack(dest)
        go(dest, me).start()
        return c

    lax.fori_loop(1, n, dispatch, 0)

    def tell(i, c):
        count(lax.rem(me + i, n), me).start()
        return c

    lax.fori_loop(1, n, tell, 0)
    count_all[me] = counts[...]
    arrived[me] = pack(me)

    for copy in weights:
        copy.wait()

    def ffn(source):
        rows = arrived[source]
        gate = jnp.dot(rows, gate_ref[...], preferred_element_type=F32)
        up = jnp.dot(rows, up_ref[...], preferred_element_type=F32)
        hidden = (gate / (1.0 + jnp.exp(-gate)) * up).astype(BF16)
        return jnp.dot(hidden, down_ref[...], preferred_element_type=F32).astype(BF16)

    def expert_step(i, c):
        source = lax.rem(me + n - spread(i, n), n)

        @pl.when(i > 0)
        def _():
            go(me, source).wait_recv()

        results[source] = ffn(source)

        @pl.when(i > 0)
        def _():
            back(source, me).start()

        return c

    lax.fori_loop(0, n, expert_step, 0)

    def heard(i, c):
        count(me, lax.rem(me + i, n)).wait_recv()
        return c

    lax.fori_loop(1, n, heard, 0)

    def add(i, carry):
        inner, whole = carry
        here = count_all[i]
        return inner + here * (i < me).astype(jnp.int32), whole + here

    zero = jnp.zeros((n, LANES), jnp.int32)
    inner, whole = lax.fori_loop(0, n, add, (zero, zero))
    totals[...] = whole

    def tell_dp(i, c):
        total(lax.rem(group + i, dps), group).start()
        return c

    lax.fori_loop(1, dps, tell_dp, 0)
    total_all[group] = whole

    def heard_dp(i, c):
        total(group, lax.rem(group + i, dps)).wait_recv()
        return c

    lax.fori_loop(1, dps, heard_dp, 0)

    def add_dp(i, outer):
        return outer + total_all[i] * (i < group).astype(jnp.int32)

    offset[...] = inner + lax.fori_loop(0, dps, add_dp, zero)
    slot_ref[...] = (
        jnp.sum(
            hot_row * offset[:, 0:1].astype(F32), axis=0, keepdims=True
        ).astype(jnp.int32)
        + rank_row
    )

    piece = min(width, 512)

    def combine(source, block, first):
        lane = lax.broadcasted_iota(jnp.int32, (tok, most), 1)
        fits = offset[pl.ds(source, 1), 0:most] + lax.broadcasted_iota(
            jnp.int32, (1, most), 1
        ) < capacity
        pick = (lane + source * most == position[...]) & fits
        pick = pick.astype(F32).astype(BF16)
        for at in range(0, width, piece):
            part = jnp.dot(
                pick, block[source, :, at : at + piece], preferred_element_type=F32
            ).astype(BF16)
            if first:
                out_ref[:, at : at + piece] = part
            else:
                out_ref[:, at : at + piece] += part

    combine(me, results, True)

    def combine_step(i, c):
        source = lax.rem(me + n - spread(i, n), n)
        back(me, source).wait_recv()
        combine(source, returned, False)
        return c

    lax.fori_loop(1, n, combine_step, 0)

    def drain(i, c):
        other = lax.rem(me + i, n)
        go(other, me).wait_send()
        back(other, me).wait_send()
        count(other, me).wait_send()
        return c

    lax.fori_loop(1, n, drain, 0)

    def drain_dp(i, c):
        total(lax.rem(group + i, dps), group).wait_send()
        return c

    lax.fori_loop(1, dps, drain_dp, 0)


def direct(tokens, expert_ids, gate_proj, up_proj, down_proj):
    tok, width = tokens.shape
    hidden = gate_proj.shape[2]
    n = lax.axis_size("expert")
    dps = lax.axis_size("dp")
    most = 2 * tok // n
    capacity = tok * dps
    vmem = pl.BlockSpec(memory_space=pltpu.VMEM)
    anywhere = pl.BlockSpec(memory_space=pltpu.MemorySpace.HBM)
    dma = pltpu.SemaphoreType.DMA
    block = pltpu.VMEM((n, most, width), BF16)
    mixed, slot = pl.pallas_call(
        functools.partial(direct_kernel, n, dps, most, capacity),
        out_shape=(
            jax.ShapeDtypeStruct((tok, width), BF16),
            jax.ShapeDtypeStruct((1, tok), jnp.int32),
        ),
        in_specs=[vmem, vmem, vmem, anywhere, anywhere, anywhere],
        out_specs=(vmem, vmem),
        scratch_shapes=[
            pltpu.VMEM((width, hidden), BF16),
            pltpu.VMEM((width, hidden), BF16),
            pltpu.VMEM((hidden, width), BF16),
            block, block, block, block,
            pltpu.VMEM((tok, 1), jnp.int32),
            pltpu.VMEM((n, LANES), jnp.int32),
            pltpu.VMEM((n, LANES), jnp.int32),
            pltpu.VMEM((n, n, LANES), jnp.int32),
            pltpu.VMEM((n, LANES), jnp.int32),
            pltpu.VMEM((dps, n, LANES), jnp.int32),
            dma((3,)), dma((n,)), dma((n,)), dma((n,)), dma((n,)),
            dma((n,)), dma((n,)), dma((dps,)), dma((dps,)),
        ],
        compiler_params=pltpu.CompilerParams(
            collective_id=0, has_side_effects=True, vmem_limit_bytes=60 * 2**20
        ),
    )(
        expert_ids.reshape(1, tok), expert_ids, tokens, gate_proj, up_proj, down_proj
    )
    return mixed, slot.reshape(tok)


def entering(part, axis, combine, identity):
    place = lax.axis_index(axis)
    gathered = lax.all_gather(part, axis)
    state = jnp.zeros_like(part) + jnp.asarray(identity, part.dtype)

    def one(hop, state):
        return combine(state, lax.dynamic_index_in_dim(gathered, hop, 0, False))

    return lax.fori_loop(0, place, one, state)


def add_counts(earlier, later):
    return earlier + later


def expert_ffn(rows, gate_proj, up_proj, down_proj):
    gate_val = jnp.dot(rows, gate_proj[0], preferred_element_type=jnp.float32)
    up_val = jnp.dot(rows, up_proj[0], preferred_element_type=jnp.float32)
    hidden = (jax.nn.silu(gate_val) * up_val).astype(jnp.bfloat16)
    return jnp.dot(hidden, down_proj[0], preferred_element_type=jnp.float32).astype(jnp.bfloat16)


def padded(tokens, expert_ids, gate_proj, up_proj, down_proj):
    tok_rows, width = tokens.shape
    experts_all = lax.axis_size("expert")
    most = 2 * tok_rows // experts_all
    capacity = tok_rows * lax.axis_size("dp")
    choices = expert_ids[:, 0]
    onehot = (choices[:, None] == jnp.arange(experts_all, dtype=jnp.int32)[None, :]).astype(
        jnp.int32
    )
    counts = jnp.sum(onehot, axis=0)
    inner = entering(counts, "expert", add_counts, jnp.zeros_like(counts))
    totals = lax.psum(counts, "expert")
    outer = entering(totals, "dp", add_counts, jnp.zeros_like(totals))
    offset = inner + outer
    before = jnp.cumsum(onehot, axis=0) - onehot
    local_rank = jnp.sum(before * onehot, axis=1)
    global_slot = (jnp.sum(onehot * offset[None, :], axis=1) + local_rank).astype(jnp.int32)
    is_kept = global_slot < capacity
    position = choices * most + local_rank
    targets = jnp.arange(experts_all * most, dtype=jnp.int32)
    dispatch = ((targets[:, None] == position[None, :]) & is_kept[None, :]).astype(jnp.bfloat16)
    outgoing = jnp.dot(dispatch, tokens, preferred_element_type=jnp.float32).astype(jnp.bfloat16)
    outgoing = outgoing.reshape(experts_all, most, width)
    arrived = lax.all_to_all(outgoing, "expert", split_axis=0, concat_axis=0, tiled=True)
    sources, slots_here, _ = arrived.shape
    flat = arrived.reshape(sources * slots_here, width)
    returned = lax.all_to_all(
        expert_ffn(flat, gate_proj, up_proj, down_proj).reshape(sources, slots_here, width),
        "expert",
        split_axis=0,
        concat_axis=0,
        tiled=True,
    )
    flat_back = returned.reshape(experts_all * most, width)
    mixed = lax.dot_general(
        dispatch, flat_back, (((0,), (0,)), ((), ())), preferred_element_type=jnp.float32
    )
    return (mixed.astype(jnp.bfloat16), global_slot)


def relay_kernel(
    n, dps, most, base, dense, capacity,
    row_ids, col_ids, tok_ref, gate_hbm, up_hbm, down_hbm,
    out_ref, slot_ref, flag_ref,
    gate_ref, up_ref, down_ref, outgoing, arrived, results, returned,
    x_out, x_in, x_back, x_home, relay_out, relay_in,
    position, x_position, offset, x_first, x_size, r_first, r_size,
    counts, count_all, totals, total_all,
    weight_sem, go_send, go_recv, back_send, back_recv,
    over_send, over_recv, gather_send, gather_recv, x_send, x_recv,
    count_send, count_recv, total_send, total_recv,
):
    me = lax.axis_index("expert")
    group = lax.axis_index("dp")
    tok, width = tok_ref.shape
    hn = n // 2
    over = most - base
    near = lax.div(me, hn) * hn
    far = hn - near
    place = me - near
    partner = far + place
    piece = min(width, 512)

    def around(i):
        return lax.rem(place + i, hn)

    weights = [
        pltpu.make_async_copy(src.at[0], dst, weight_sem.at[i])
        for i, (src, dst) in enumerate(
            ((gate_hbm, gate_ref), (up_hbm, up_ref), (down_hbm, down_ref))
        )
    ]
    for copy in weights:
        copy.start()

    barrier = pltpu.get_barrier_semaphore()

    def greet(i, c):
        pl.semaphore_signal(
            barrier, inc=1, device_id={"expert": lax.rem(me + i, n)}, device_id_type=MESH
        )
        return c

    def greet_dp(i, c):
        pl.semaphore_signal(
            barrier, inc=1, device_id={"dp": lax.rem(group + i, dps)}, device_id_type=MESH
        )
        return c

    lax.fori_loop(1, n, greet, 0)
    lax.fori_loop(1, dps, greet_dp, 0)

    def iota(shape, axis):
        return lax.broadcasted_iota(jnp.int32, shape, axis)

    def ones(mask):
        return mask.astype(F32).astype(BF16)

    def dot(a, b):
        return jnp.dot(a, b, preferred_element_type=F32)

    def excess(count, half):
        rows = iota((n, LANES), 0)
        inside = (rows >= half) & (rows < half + hn)
        size = jnp.where(inside, jnp.maximum(count - base, 0), 0)
        first = dot(
            ones(iota((n, n), 1) < iota((n, n), 0)), size.astype(F32).astype(BF16)
        ).astype(jnp.int32)
        return first, size

    ids_row = row_ids[...]
    hot_row = (ids_row == iota((n, tok), 0)).astype(F32)
    before_row = dot(hot_row.astype(BF16), ones(iota((tok, tok), 0) < iota((tok, tok), 1)))
    rank_row = jnp.sum(before_row * hot_row, axis=0, keepdims=True).astype(jnp.int32)
    pos_row = ids_row * most + rank_row
    mine = jnp.broadcast_to(
        jnp.sum(hot_row, axis=1, keepdims=True), (n, LANES)
    ).astype(jnp.int32)
    counts[...] = mine
    first, size = excess(mine, far)
    x_first[...] = first
    x_size[...] = size
    start_row = jnp.sum(
        hot_row * x_first[:, 0:1].astype(F32), axis=0, keepdims=True
    ).astype(jnp.int32)
    x_row = jnp.where(
        (ids_row >= far) & (ids_row < far + hn) & (rank_row >= base),
        start_row + rank_row - base, -1,
    )

    ids_col = col_ids[...]
    hot_col = (ids_col == iota((tok, n), 1)).astype(F32)

    def go(dest, source, far_off):
        rows = pl.ds(0, base if far_off else most)
        return pltpu.make_async_remote_copy(
            src_ref=outgoing.at[dest, rows], dst_ref=arrived.at[source, rows],
            send_sem=go_send.at[dest], recv_sem=go_recv.at[source],
            device_id={"expert": dest}, device_id_type=MESH,
        )

    def back(dest, source, far_off):
        rows = pl.ds(0, base if far_off else most)
        return pltpu.make_async_remote_copy(
            src_ref=results.at[dest, rows], dst_ref=returned.at[source, rows],
            send_sem=back_send.at[dest], recv_sem=back_recv.at[source],
            device_id={"expert": dest}, device_id_type=MESH,
        )

    def forward(dest, slot, source):
        return pltpu.make_async_remote_copy(
            src_ref=relay_out.at[slot], dst_ref=arrived.at[source, pl.ds(base, over)],
            send_sem=over_send.at[slot], recv_sem=over_recv.at[source],
            device_id={"expert": dest}, device_id_type=MESH,
        )

    def gather(dest, source, slot):
        return pltpu.make_async_remote_copy(
            src_ref=results.at[source, pl.ds(base, over)], dst_ref=relay_in.at[slot],
            send_sem=gather_send.at[source], recv_sem=gather_recv.at[slot],
            device_id={"expert": dest}, device_id_type=MESH,
        )

    def cross(which, src, dst):
        return pltpu.make_async_remote_copy(
            src_ref=src, dst_ref=dst,
            send_sem=x_send.at[which], recv_sem=x_recv.at[which],
            device_id={"expert": partner}, device_id_type=MESH,
        )

    def count(dest, source):
        return pltpu.make_async_remote_copy(
            src_ref=counts, dst_ref=count_all.at[source],
            send_sem=count_send.at[dest], recv_sem=count_recv.at[source],
            device_id={"expert": dest}, device_id_type=MESH,
        )

    def total(dest, source):
        return pltpu.make_async_remote_copy(
            src_ref=totals, dst_ref=total_all.at[source],
            send_sem=total_send.at[dest], recv_sem=total_recv.at[source],
            device_id={"dp": dest}, device_id_type=MESH,
        )

    def pack(dest, rows):
        pick = ones(iota((rows, tok), 0) + dest * most == pos_row)
        return dot(pick, tok_ref[...]).astype(BF16)

    x_out[...] = dot(ones(iota((dense, tok), 0) == x_row), tok_ref[...]).astype(BF16)

    pl.semaphore_wait(barrier, n + dps - 2)

    def tell(i, c):
        count(lax.rem(me + i, n), me).start()
        return c

    lax.fori_loop(1, n, tell, 0)
    send_x = cross(0, x_out, x_in)
    send_x.start()

    def dispatch_near(i, c):
        dest = near + around(i)
        outgoing[dest] = pack(dest, most)
        go(dest, me, False).start()
        return c

    lax.fori_loop(1, hn, dispatch_near, 0)

    def dispatch_far(i, c):
        dest = far + around(i)
        outgoing[dest, pl.ds(0, base)] = pack(dest, base)
        go(dest, me, True).start()
        return c

    lax.fori_loop(0, hn, dispatch_far, 0)
    count_all[me] = mine
    arrived[me] = pack(me, most)

    before_col = dot(ones(iota((tok, tok), 0) > iota((tok, tok), 1)), hot_col.astype(BF16))
    rank_col = jnp.sum(before_col * hot_col, axis=1, keepdims=True).astype(jnp.int32)
    position[...] = ids_col * most + rank_col
    lane = iota((1, n), 1)
    size_lane = jnp.where(
        (lane >= far) & (lane < far + hn),
        jnp.maximum(jnp.sum(hot_col, axis=0, keepdims=True) - base, 0.0), 0.0,
    )
    first_lane = dot(
        jnp.broadcast_to(size_lane, (16, n)).astype(BF16),
        ones(iota((n, n), 0) < iota((n, n), 1)),
    )[0:1]
    start_col = jnp.sum(hot_col * first_lane, axis=1, keepdims=True).astype(jnp.int32)
    x_position[...] = jnp.where(
        (ids_col >= far) & (ids_col < far + hn) & (rank_col >= base),
        start_col + rank_col - base, -1,
    )

    for copy in weights:
        copy.wait()

    def ffn(source):
        rows = arrived[source]
        gate = dot(rows, gate_ref[...])
        up = dot(rows, up_ref[...])
        hidden = (gate / (1.0 + jnp.exp(-gate)) * up).astype(BF16)
        results[source] = dot(hidden, down_ref[...]).astype(BF16)

    def near_step(i, c):
        source = near + lax.rem(place + hn - i, hn)

        @pl.when(i > 0)
        def _():
            go(me, source, False).wait_recv()

        ffn(source)

        @pl.when(i > 0)
        def _():
            back(source, me, False).start()

        @pl.when(i == 0)
        def _():
            unpack()

        return c

    def unpack():
        count(me, partner).wait_recv()
        send_x.wait_recv()
        first, size = excess(count_all[partner], near)
        r_first[...] = first
        r_size[...] = size

        def one(i, c):
            slot = around(i)
            dest = near + slot
            row = iota((over, dense), 0)
            pick = (iota((over, dense), 1) == row + r_first[pl.ds(dest, 1), 0:1]) & (
                row < r_size[pl.ds(dest, 1), 0:1]
            )
            block = dot(ones(pick), x_in[...]).astype(BF16)

            @pl.when(i == 0)
            def _():
                arrived[partner, pl.ds(base, over)] = block

            @pl.when(i > 0)
            def _():
                relay_out[slot] = block
                forward(dest, slot, partner).start()

            return c

        lax.fori_loop(0, hn, one, 0)

    lax.fori_loop(0, hn, near_step, 0)

    def far_step(i, c):
        slot = lax.rem(place + hn - i, hn)
        source = far + slot
        go(me, source, True).wait_recv()

        @pl.when(i > 0)
        def _():
            forward(me, place, source).wait_recv()

        ffn(source)
        back(source, me, True).start()

        @pl.when(i > 0)
        def _():
            gather(near + slot, source, place).start()

        @pl.when(i == 0)
        def _():
            relay_in[place] = results[source, pl.ds(base, over)]

        return c

    lax.fori_loop(0, hn, far_step, 0)

    def collect(i, c):
        gather(me, partner, around(i)).wait_recv()
        return c

    lax.fori_loop(1, hn, collect, 0)
    picks = []
    for slot in range(hn):
        column = iota((dense, over), 1)
        pick = (
            iota((dense, over), 0) == column + r_first[pl.ds(near + slot, 1), 0:1]
        ) & (column < r_size[pl.ds(near + slot, 1), 0:1])
        picks.append(ones(pick))
    for at in range(0, width, piece):
        acc = dot(picks[0], relay_in[0, :, at : at + piece])
        for slot in range(1, hn):
            acc += dot(picks[slot], relay_in[slot, :, at : at + piece])
        x_back[:, at : at + piece] = acc.astype(BF16)
    send_back = cross(1, x_back, x_home)
    send_back.start()

    def heard(i, c):
        @pl.when(i != hn)
        def _():
            count(me, lax.rem(me + i, n)).wait_recv()

        return c

    lax.fori_loop(1, n, heard, 0)

    def add(i, carry):
        inner, whole, need = carry
        here = count_all[i]
        other = hn - lax.div(i, hn) * hn
        rows = iota((n, LANES), 0)
        outside = (rows >= other) & (rows < other + hn)
        extra = jnp.sum(
            jnp.where(outside, jnp.maximum(here - base, 0), 0), axis=0, keepdims=True
        )
        return (
            inner + here * (i < me).astype(jnp.int32), whole + here, jnp.maximum(need, extra)
        )

    zero = jnp.zeros((n, LANES), jnp.int32)
    inner, whole, need = lax.fori_loop(
        0, n, add, (zero, zero, jnp.zeros((1, LANES), jnp.int32))
    )
    need = jnp.broadcast_to(need, (8, LANES))
    totals[0] = whole
    totals[1] = need

    def tell_dp(i, c):
        total(lax.rem(group + i, dps), group).start()
        return c

    lax.fori_loop(1, dps, tell_dp, 0)
    total_all[group, 0] = whole
    total_all[group, 1] = need

    def heard_dp(i, c):
        total(group, lax.rem(group + i, dps)).wait_recv()
        return c

    lax.fori_loop(1, dps, heard_dp, 0)

    def add_dp(i, carry):
        outer, most_needed = carry
        return (
            outer + total_all[i, 0] * (i < group).astype(jnp.int32),
            jnp.maximum(most_needed, total_all[i, 1]),
        )

    outer, needed = lax.fori_loop(0, dps, add_dp, (zero, need))
    offset[...] = inner + outer
    flag_ref[...] = (needed > dense).astype(jnp.int32)
    slot_ref[...] = (
        jnp.sum(hot_row * offset[:, 0:1].astype(F32), axis=0, keepdims=True).astype(jnp.int32)
        + rank_row
    )

    def combine(pick, block, first):
        for at in range(0, width, piece):
            part = dot(pick, block[:, at : at + piece]).astype(BF16)
            if first:
                out_ref[:, at : at + piece] = part
            else:
                out_ref[:, at : at + piece] += part

    def choose(source, rows):
        fits = offset[pl.ds(source, 1), 0:rows] + iota((1, rows), 1) < capacity
        return ones((iota((tok, rows), 1) + source * most == position[...]) & fits)

    combine(choose(me, most), results.at[me], True)

    def near_back(i, c):
        source = near + lax.rem(place + hn - i, hn)
        back(me, source, False).wait_recv()
        combine(choose(source, most), returned.at[source], False)
        return c

    lax.fori_loop(1, hn, near_back, 0)

    def far_back(i, c):
        source = far + lax.rem(place + hn - i, hn)
        back(me, source, True).wait_recv()
        combine(choose(source, base), returned.at[source, pl.ds(0, base)], False)
        return c

    lax.fori_loop(0, hn, far_back, 0)

    entry = iota((1, dense), 1)
    keep = jnp.zeros((1, dense), jnp.int32)
    for slot in range(hn):
        row = pl.ds(far + slot, 1)
        rank = entry - x_first[row, 0:1]
        inside = (rank >= 0) & (rank < x_size[row, 0:1])
        keep += (inside & (offset[row, 0:1] + rank + base < capacity)).astype(jnp.int32)
    send_back.wait_recv()
    combine(
        ones((iota((tok, dense), 1) == x_position[...]) & (keep > 0)), x_home, False
    )

    send_x.wait_send()
    send_back.wait_send()

    def drain_near(i, c):
        slot = around(i)
        other = near + slot
        go(other, me, False).wait_send()
        back(other, me, False).wait_send()
        forward(other, slot, partner).wait_send()
        gather(other, far + slot, place).wait_send()
        return c

    lax.fori_loop(1, hn, drain_near, 0)

    def drain_far(i, c):
        other = far + i
        go(other, me, True).wait_send()
        back(other, me, True).wait_send()
        return c

    lax.fori_loop(0, hn, drain_far, 0)

    def drain(i, c):
        count(lax.rem(me + i, n), me).wait_send()
        return c

    lax.fori_loop(1, n, drain, 0)

    def drain_dp(i, c):
        total(lax.rem(group + i, dps), group).wait_send()
        return c

    lax.fori_loop(1, dps, drain_dp, 0)


def relayed(tokens, expert_ids, gate_proj, up_proj, down_proj):
    tok, width = tokens.shape
    hidden = gate_proj.shape[2]
    n = lax.axis_size("expert")
    dps = lax.axis_size("dp")
    most = 2 * tok // n
    base = 3 * most // 8
    over = most - base
    dense = 13 * most // 8
    capacity = tok * dps
    vmem = pl.BlockSpec(memory_space=pltpu.VMEM)
    anywhere = pl.BlockSpec(memory_space=pltpu.MemorySpace.HBM)
    dma = pltpu.SemaphoreType.DMA
    block = pltpu.VMEM((n, most, width), BF16)
    packed = pltpu.VMEM((dense, width), BF16)
    relay = pltpu.VMEM((n // 2, over, width), BF16)
    table = pltpu.VMEM((n, LANES), jnp.int32)
    column = pltpu.VMEM((tok, 1), jnp.int32)
    mixed, slot, flag = pl.pallas_call(
        functools.partial(relay_kernel, n, dps, most, base, dense, capacity),
        out_shape=(
            jax.ShapeDtypeStruct((tok, width), BF16),
            jax.ShapeDtypeStruct((1, tok), jnp.int32),
            jax.ShapeDtypeStruct((8, LANES), jnp.int32),
        ),
        in_specs=[vmem, vmem, vmem, anywhere, anywhere, anywhere],
        out_specs=(vmem, vmem, vmem),
        scratch_shapes=[
            pltpu.VMEM((width, hidden), BF16),
            pltpu.VMEM((width, hidden), BF16),
            pltpu.VMEM((hidden, width), BF16),
            block, block, block, block,
            packed, packed, packed, packed, relay, relay,
            column, column, table, table, table, table, table,
            table,
            pltpu.VMEM((n, n, LANES), jnp.int32),
            pltpu.VMEM((2, n, LANES), jnp.int32),
            pltpu.VMEM((dps, 2, n, LANES), jnp.int32),
            dma((3,)), dma((n,)), dma((n,)), dma((n,)), dma((n,)),
            dma((n // 2,)), dma((n,)), dma((n,)), dma((n // 2,)), dma((2,)), dma((2,)),
            dma((n,)), dma((n,)), dma((dps,)), dma((dps,)),
        ],
        compiler_params=pltpu.CompilerParams(
            collective_id=0, has_side_effects=True, vmem_limit_bytes=60 * 2**20
        ),
    )(
        expert_ids.reshape(1, tok), expert_ids, tokens, gate_proj, up_proj, down_proj
    )
    return lax.cond(
        flag[0, 0] > 0,
        lambda: padded(tokens, expert_ids, gate_proj, up_proj, down_proj),
        lambda: (mixed, slot.reshape(tok)),
    )


def on_device(tokens, expert_ids, gate_proj, up_proj, down_proj):
    n = lax.axis_size("expert")
    if n == 8 and 2 * tokens.shape[0] // n % LANES == 0:
        return relayed(tokens, expert_ids, gate_proj, up_proj, down_proj)
    return direct(tokens, expert_ids, gate_proj, up_proj, down_proj)


def solution(mesh):
    in_specs = (
        P(("dp", "expert"), None),
        P(("dp", "expert"), None),
        P("expert", None, None),
        P("expert", None, None),
        P("expert", None, None),
    )
    out_specs = (P(("dp", "expert"), None), P(("dp", "expert")))
    return jax.shard_map(
        on_device, mesh=mesh, in_specs=in_specs, out_specs=out_specs, check_vma=False
    )
```
